32 devices in a mesh: node: 8 (over z, core), local: 4 (over y, x).
Axes of the slice: x: 2, y: 2, z: 4, core: 2. Of those that a mesh axis runs over, the one named last changes fastest.
Arguments:
- tokens: bfloat16 [4096, 1280], P(('node', 'local')), may hold values from -64 to 64
- modality: int32 [4096], P(('node', 'local')), may hold values from 0 to 1, as said below
- expert_id: int32 [4096], P(('node', 'local')), may hold values from 0 to 31, as said below
- slot: int32 [4096], P(('node', 'local')), may hold values from 0 to 7, as said below
- type_embed: bfloat16 [2, 1280], replicated, may hold values from -6 to 6
- router: bfloat16 [1280, 32], replicated, may hold values from -1 to 1
- w_in: bfloat16 [32, 1280, 5120], P(('node', 'local')), may hold values from -0.15625 to 0.15625
- w_out: bfloat16 [32, 5120, 1280], P(('node', 'local')), may hold values from -0.078125 to 0.078125
Outputs:
- combined: bfloat16 [4096, 1280], P(('node', 'local'))
- losses: float32 [4], replicated
The draws below stay inside these ranges and needn't reach their ends.
Inputs may be any that keep to these rules, and one draw needn't show every extreme that they name: `expert_id`: within each device's block of 128 tokens no expert is named more than 8 times, and in every draw some expert is named exactly 8 times in every block. `slot`: tokens of one device's block that name the same expert have distinct slots. `modality`: each device's block holds tokens of both modalities.
All inputs are finite; a program needn't handle non-finite values.
Results may differ from the reference program's by a relative error of at most 0.0095.
Values may be sent and summed in bfloat16 or wider, within the bound.
A program may use at most 64 MiB of HBM per device.

```python
import jax
import jax.numpy as jnp
from jax import lax

D = 1280
FF = 5120
EXPERTS = 32
TOK_DEV = 128
CAP = 8
SHARDS = 1
TOKENS = 4096


def routing_pair(key):
    base = jax.random.fold_in(key, 11)
    blocks = TOKENS // TOK_DEV
    slots_all = EXPERTS * CAP
    fullest = jax.random.randint(jax.random.fold_in(base, 1), (), 0, EXPERTS)
    block_keys = jax.random.split(jax.random.fold_in(base, 2), blocks)

    def one_block(block_key):
        first_key, second_key = jax.random.split(block_key)
        ranking = jax.random.permutation(first_key, slots_all)
        owner = jnp.arange(slots_all) // CAP
        score = jnp.where(owner == fullest, ranking - slots_all, ranking)
        order = jnp.argsort(score, stable=True)[:TOK_DEV]
        return jax.random.permutation(second_key, order)
    chosen = jax.vmap(one_block)(block_keys).reshape(-1)
    return ((chosen // CAP).astype(jnp.int32), (chosen % CAP).astype(jnp.int32))


def joint_draw(key):
    blocks = TOKENS // TOK_DEV
    router = jnp.clip(jax.random.normal(jax.random.fold_in(key, 21), (D, EXPERTS), jnp.float32) * D ** (-0.5), -1.0, 1.0)
    embed = jnp.clip(jax.random.normal(jax.random.fold_in(key, 22), (2, D), jnp.float32), -6.0, 6.0)
    block_index = jnp.arange(blocks)
    ones_count = TOK_DEV // 4 + TOK_DEV // 2 * block_index // max(blocks - 1, 1)
    ranking = jax.vmap(lambda sub: jax.random.permutation(sub, TOK_DEV))(jax.random.split(jax.random.fold_in(key, 23), blocks))
    modality = (ranking < ones_count[:, None]).astype(jnp.int32).reshape(-1)
    values = jax.random.normal(jax.random.fold_in(key, 24), (TOKENS, D), jnp.float32)
    tokens = jnp.clip(values, -64.0, 64.0)
    return (tokens, modality, router, embed)


def draw_tokens(key, part):
    return joint_draw(key)[0].astype(jnp.bfloat16)


def draw_modality(key, part):
    return joint_draw(key)[1]


def draw_router(key, part):
    return joint_draw(key)[2].astype(jnp.bfloat16)


def draw_type_embed(key, part):
    return joint_draw(key)[3].astype(jnp.bfloat16)


def draw_expert_id(key, part):
    return routing_pair(key)[0]


def draw_slot(key, part):
    return routing_pair(key)[1]


def steps_of(stream_key, extent, pieces, least, high):
    def one(dim, blocks):
        steps = jax.random.uniform(jax.random.fold_in(jax.random.fold_in(stream_key, 6), dim), (blocks,), jnp.float32, least / len(pieces), high / len(pieces))
        return jnp.repeat(jnp.exp(steps), extent[dim] // blocks).reshape((-1,) + (1,) * (len(extent) - dim - 1))

    level = one(*pieces[0])
    for cut in pieces[1:]:
        level = level * one(*cut)
    return level


def noise(rng, extent, spread, limit, pieces=(), held_as=jnp.bfloat16):
    factor_of = steps_of(rng, extent, pieces, -0.22, 0.18) if pieces else 1.0
    values = jax.random.normal(rng, extent, jnp.float32) * spread * factor_of
    return jnp.minimum(jnp.maximum(values, -limit), limit).astype(held_as)


def setup_inputs(seed: int = 0) -> dict:
    keys = jax.random.split(jax.random.key(seed), 9)
    return {
        "tokens": draw_tokens(jax.random.fold_in(keys[8], 71), 0),
        "modality": draw_modality(jax.random.fold_in(keys[8], 71), 0),
        "expert_id": draw_expert_id(jax.random.fold_in(keys[8], 71), 0),
        "slot": draw_slot(jax.random.fold_in(keys[8], 71), 0),
        "type_embed": draw_type_embed(jax.random.fold_in(keys[8], 71), 0),
        "router": draw_router(jax.random.fold_in(keys[8], 71), 0),
        "w_in": noise(keys[6], (EXPERTS * SHARDS, D, FF // SHARDS), D ** -0.5, 0.15625, ((0, 32),)),
        "w_out": noise(keys[7], (EXPERTS * SHARDS, FF // SHARDS, D), FF ** -0.5, 0.078125, ((0, 32),)),
    }


def reference(tokens, modality, expert_id, slot, type_embed, router, w_in, w_out):
    picked = jnp.where(modality[:, None] == 1, type_embed[1].astype(jnp.float32)[None, :], type_embed[0].astype(jnp.float32)[None, :])
    mixed = (tokens.astype(jnp.float32) + picked).astype(jnp.bfloat16)
    logits = jnp.dot(mixed, router, preferred_element_type=jnp.float32)
    logp = jax.nn.log_softmax(logits, axis=-1)
    probs = jnp.exp(logp)
    entropy = -jnp.sum(probs * logp, axis=-1)
    gate = jnp.take_along_axis(probs, expert_id[:, None].astype(jnp.int32), axis=1)[:, 0]
    blocks = TOKENS // TOK_DEV
    total_rows = blocks * CAP
    position = (jnp.arange(TOKENS, dtype=jnp.int32) // TOK_DEV) * CAP + slot

    def one_expert(expert):
        index = jnp.where(expert_id == expert, position, total_rows).astype(jnp.int32)
        rows = jnp.zeros((total_rows, D), jnp.bfloat16).at[index].set(mixed, mode="drop")
        total = jnp.zeros((total_rows, D), jnp.float32)
        for block in range(SHARDS):
            first = w_in[expert * SHARDS + block]
            second = w_out[expert * SHARDS + block]
            hidden = jax.nn.gelu(jnp.dot(rows, first, preferred_element_type=jnp.float32), approximate=False).astype(jnp.bfloat16)
            part = jnp.dot(hidden, second, preferred_element_type=jnp.float32).astype(jnp.bfloat16)
            total = total + part.astype(jnp.float32)
        return total

    outputs = lax.map(one_expert, jnp.arange(EXPERTS, dtype=jnp.int32))
    picked_rows = outputs[expert_id, position]
    combined = (EXPERTS * gate[:, None] * picked_rows).astype(jnp.bfloat16)
    member = jnp.stack([modality == 0, modality == 1], axis=1).astype(jnp.float32)
    counts = jnp.sum(member, axis=0)
    prob_sum = jnp.dot(member.T, probs, precision=lax.Precision.HIGHEST)
    entropy_sum = jnp.dot(member.T, entropy, precision=lax.Precision.HIGHEST)
    local_part = entropy_sum / counts
    mean_prob = prob_sum / counts[:, None]
    global_part = jnp.sum(mean_prob * jnp.log(mean_prob), axis=1)
    losses = jnp.concatenate([local_part, global_part])
    return combined, losses
```

```python
import functools

import jax
import jax.numpy as jnp
from jax import lax
from jax.experimental import pallas as pl
from jax.experimental.pallas import tpu as pltpu
from jax.sharding import PartitionSpec as P

CAP = 8
LANES = 128
GROUPS = 2
MESH = pl.DeviceIdType.MESH


def tile_of(size, widest):
    tile = widest
    while size % tile:
        tile //= 2
    return tile


def gelu(x):
    half = 0.5 * x
    return half + half * lax.erf(x * 0.7071067811865476)


def column(row):
    size = row.shape[1]
    return jnp.transpose(jnp.broadcast_to(row, (size, size)))[:, :1]


def kernel(
    nodes, locals_, shards, experts, groups, hidden_tile, cols, weight_cuts,
    tok_hbm, ids_hbm, emb_hbm, router_hbm, w1_hbm, w2_hbm,
    out_ref, loss_ref,
    tok, ids, emb, router, w1, w2, stage, recv, hid, back, ret, stats, all_stats,
    in_sem, w1_sem, w2_sem, go_sem, got_sem, back_sem, ret_sem, stat_send, stat_recv,
):
    devices = nodes * locals_
    half = devices // groups
    width = tok.shape[1]
    count = tok.shape[0]
    chunks = width // cols
    me_n = lax.axis_index("node")
    me_l = lax.axis_index("local")
    me = me_n * locals_ + me_l
    my_pos = (me_n // groups) * locals_ + me_l

    def for_group(group, body):
        def step(i, _):
            peer_n = lax.rem(me_n + (i // locals_) * groups + group, nodes)
            peer_l = lax.rem(me_l + lax.rem(i, locals_), locals_)
            body(peer_n, peer_l)
            return 0

        lax.fori_loop(1 if group == 0 else 0, half, step, 0)

    def all_peers(body):
        for group in range(groups):
            for_group(group, body)

    barrier = pltpu.get_barrier_semaphore()
    all_peers(
        lambda n, l: pl.semaphore_signal(barrier, inc=1, device_id=(n, l), device_id_type=MESH)
    )
    loads = [
        pltpu.make_async_copy(src, dst, in_sem.at[i])
        for i, (src, dst) in enumerate(
            ((ids_hbm, ids), (emb_hbm, emb), (tok_hbm, tok), (router_hbm, router))
        )
    ]
    for load in loads:
        load.start()
    weight_loads = []
    for hbm, vmem, sem in ((w1_hbm, w1, w1_sem), (w2_hbm, w2, w2_sem)):
        rows = vmem.shape[0] // weight_cuts
        weight_loads.append(
            [
                pltpu.make_async_copy(
                    hbm.at[0, pl.ds(i * rows, rows)], vmem.at[pl.ds(i * rows, rows)], sem.at[i]
                )
                for i in range(weight_cuts)
            ]
        )
        for load in weight_loads[-1]:
            load.start()
    for load in loads:
        load.wait()

    modality = ids[0:1, :]
    expert_id = ids[1:2, :]
    slot = ids[2:3, :]
    is_text = column(modality) == 1
    picked = jnp.where(
        is_text, emb[1:2, :].astype(jnp.float32), emb[0:1, :].astype(jnp.float32)
    )
    mixed = (tok[...].astype(jnp.float32) + picked).astype(jnp.bfloat16)
    place = lax.broadcasted_iota(jnp.int32, (experts * CAP, count), 0)
    select = (place == expert_id * CAP + slot).astype(jnp.bfloat16)
    stage[...] = (
        jnp.dot(select, mixed, preferred_element_type=jnp.float32)
        .reshape(experts, CAP, width)
        .astype(jnp.bfloat16)
    )

    pl.semaphore_wait(barrier, devices - 1)

    for group in range(groups):
        if group == 0:
            pltpu.make_async_copy(
                stage.at[me // shards], recv.at[0, my_pos], got_sem.at[0]
            ).start()

        def dispatch(n, l):
            pltpu.make_async_remote_copy(
                src_ref=stage.at[(n * locals_ + l) // shards],
                dst_ref=recv.at[group, my_pos],
                send_sem=go_sem.at[group],
                recv_sem=got_sem.at[group],
                device_id=(n, l),
                device_id_type=MESH,
            ).start()

        for_group(group, dispatch)

    logits = jnp.dot(mixed, router[...], preferred_element_type=jnp.float32)
    shifted = logits - jnp.max(logits, axis=-1, keepdims=True)
    logp = shifted - jnp.log(jnp.sum(jnp.exp(shifted), axis=-1, keepdims=True))
    probs = jnp.exp(logp)
    entropy = -jnp.sum(probs * logp, axis=-1, keepdims=True)
    expert_col = column(expert_id)
    lane = lax.broadcasted_iota(jnp.int32, (count, experts), 1)
    gate = jnp.sum(jnp.where(lane == expert_col, probs, 0.0), axis=1, keepdims=True)
    stats[...] = jnp.zeros_like(stats)
    for m in range(2):
        member = is_text if m == 1 else jnp.logical_not(is_text)
        stats[m : m + 1, 0:experts] = jnp.sum(
            jnp.where(member, probs, 0.0), axis=0, keepdims=True
        )
        stats[m : m + 1, experts : experts + 1] = jnp.sum(
            jnp.where(member, entropy, 0.0), axis=0, keepdims=True
        )
        stats[m : m + 1, experts + 1 : experts + 2] = jnp.sum(
            jnp.where(member, 1.0, 0.0), axis=0, keepdims=True
        )
    scale = experts * gate
    spot = lax.broadcasted_iota(jnp.int32, (count, devices * CAP), 1)
    first = expert_col * (shards * CAP) + column(slot)
    found = spot == first
    for s in range(1, shards):
        found = jnp.logical_or(found, spot == first + s * CAP)
    pick = found.astype(jnp.bfloat16)

    pltpu.make_async_copy(stats, all_stats.at[me], stat_recv).start()
    all_peers(
        lambda n, l: pltpu.make_async_remote_copy(
            src_ref=stats,
            dst_ref=all_stats.at[me],
            send_sem=stat_send,
            recv_sem=stat_recv,
            device_id=(n, l),
            device_id_type=MESH,
        ).start()
    )

    for group in range(groups):
        pltpu.make_async_copy(recv.at[group], recv.at[group], got_sem.at[group]).wait()
        rows = recv[group].astype(jnp.float32).reshape(half * CAP, width).astype(jnp.bfloat16)
        if group == 0:
            for load in weight_loads[0]:
                load.wait()

        def first_layer(i, _):
            at = pl.ds(pl.multiple_of(i * hidden_tile, hidden_tile), hidden_tile)
            hid[:, at] = gelu(
                jnp.dot(rows, w1[:, at], preferred_element_type=jnp.float32)
            ).astype(jnp.bfloat16)
            return 0

        lax.fori_loop(0, hid.shape[1] // hidden_tile, first_layer, 0)
        if group == 0:
            for load in weight_loads[1]:
                load.wait()

        def second_layer(c, _):
            at = pl.ds(pl.multiple_of(c * cols, cols), cols)
            back[group, c] = (
                jnp.dot(hid[...], w2[:, at], preferred_element_type=jnp.float32)
                .reshape(half, CAP, cols)
                .astype(jnp.bfloat16)
            )
            if group == 0:
                pltpu.make_async_copy(
                    back.at[0, c, my_pos], ret.at[c, me], ret_sem.at[0, c]
                ).start()

            def give(n, l):
                pltpu.make_async_remote_copy(
                    src_ref=back.at[group, c, (n // groups) * locals_ + l],
                    dst_ref=ret.at[c, me],
                    send_sem=back_sem.at[group, c],
                    recv_sem=ret_sem.at[group, c],
                    device_id=(n, l),
                    device_id_type=MESH,
                ).start()

            for_group(group, give)
            return 0

        lax.fori_loop(0, chunks, second_layer, 0)

    pltpu.make_async_copy(all_stats, all_stats, stat_recv).wait()
    total = jnp.sum(all_stats[...], axis=0)
    tokens_of = total[:, experts + 1 : experts + 2]
    entropy_mean = total[:, experts : experts + 1] / tokens_of
    mean = total[:, 0:experts] / tokens_of
    spread = jnp.sum(mean * jnp.log(mean), axis=1, keepdims=True)
    loss_ref[0] = entropy_mean[0, 0]
    loss_ref[1] = entropy_mean[1, 0]
    loss_ref[2] = spread[0, 0]
    loss_ref[3] = spread[1, 0]

    for c in range(chunks):
        for group in range(groups):
            part = ret.at[c, pl.ds(0, half)]
            pltpu.make_async_copy(part, part, ret_sem.at[group, c]).wait()
        table = (
            ret[c].astype(jnp.float32).reshape(devices * CAP, cols).astype(jnp.bfloat16)
        )
        out_ref[:, c * cols : (c + 1) * cols] = (
            scale * jnp.dot(pick, table, preferred_element_type=jnp.float32)
        ).astype(jnp.bfloat16)

    for group in range(groups):
        sent = half - 1 if group == 0 else half
        done = recv.at[group, pl.ds(0, sent)]
        pltpu.make_async_copy(done, done, go_sem.at[group]).wait()
        for c in range(chunks):
            done = back.at[group, c, pl.ds(0, sent)]
            pltpu.make_async_copy(done, done, back_sem.at[group, c]).wait()
    done = all_stats.at[pl.ds(0, devices - 1)]
    pltpu.make_async_copy(done, done, stat_send).wait()


def local(nodes, locals_, tokens, modality, expert_id, slot, type_embed, router, w_in, w_out):
    count, width = tokens.shape
    experts = router.shape[1]
    devices = nodes * locals_
    shards = devices // experts
    hidden = w_in.shape[2]
    groups = GROUPS if nodes % GROUPS == 0 else 1
    half = devices // groups
    cols = tile_of(width, 256)
    chunks = width // cols
    cuts = 5 if width % 80 == 0 and hidden % 80 == 0 else 1
    ids = jnp.stack([modality, expert_id, slot])
    bf16 = jnp.bfloat16
    any_space = pl.BlockSpec(memory_space=pl.ANY)
    dma = pltpu.SemaphoreType.DMA
    combined, losses = pl.pallas_call(
        functools.partial(
            kernel, nodes, locals_, shards, experts, groups, tile_of(hidden, 512), cols, cuts
        ),
        out_shape=(
            jax.ShapeDtypeStruct((count, width), bf16),
            jax.ShapeDtypeStruct((4,), jnp.float32),
        ),
        in_specs=[any_space] * 6,
        out_specs=(
            pl.BlockSpec(memory_space=pltpu.VMEM),
            pl.BlockSpec(memory_space=pltpu.SMEM),
        ),
        scratch_shapes=[
            pltpu.VMEM((count, width), bf16),
            pltpu.VMEM((3, count), jnp.int32),
            pltpu.VMEM((2, width), bf16),
            pltpu.VMEM((width, experts), bf16),
            pltpu.VMEM((width, hidden), bf16),
            pltpu.VMEM((hidden, width), bf16),
            pltpu.VMEM((experts, CAP, width), bf16),
            pltpu.VMEM((groups, half, CAP, width), bf16),
            pltpu.VMEM((half * CAP, hidden), bf16),
            pltpu.VMEM((groups, chunks, half, CAP, cols), bf16),
            pltpu.VMEM((chunks, devices, CAP, cols), bf16),
            pltpu.VMEM((2, LANES), jnp.float32),
            pltpu.VMEM((devices, 2, LANES), jnp.float32),
            dma((4,)),
            dma((cuts,)),
            dma((cuts,)),
            dma((groups,)),
            dma((groups,)),
            dma((groups, chunks)),
            dma((groups, chunks)),
            dma,
            dma,
        ],
        compiler_params=pltpu.CompilerParams(
            collective_id=0, has_side_effects=True, vmem_limit_bytes=62 * 1024 * 1024
        ),
    )(tokens, ids, type_embed, router, w_in, w_out)
    return combined, losses


def solution(mesh):
    placed = (
        P(("node", "local"), None),
        P(("node", "local")),
        P(("node", "local")),
        P(("node", "local")),
        P(),
        P(),
        P(("node", "local"), None, None),
        P(("node", "local"), None, None),
    )
    return jax.shard_map(
        functools.partial(local, mesh.shape["node"], mesh.shape["local"]),
        mesh=mesh,
        in_specs=placed,
        out_specs=(P(("node", "local"), None), P()),
        check_vma=False,
    )
```

```python
import functools

import jax
import jax.numpy as jnp
from jax import lax
from jax.experimental import pallas as pl
from jax.experimental.pallas import tpu as pltpu
from jax.sharding import PartitionSpec as P

CAP = 8
LANES = 128
GROUPS = 2
MESH = pl.DeviceIdType.MESH


def tile_of(size, widest):
    tile = widest
    while size % tile:
        tile //= 2
    return tile


def gelu(x):
    half = 0.5 * x
    return half + half * lax.erf(x * 0.7071067811865476)


def column(row):
    size = row.shape[1]
    return jnp.transpose(jnp.broadcast_to(row, (size, size)))[:, :1]


def kernel(
    nodes, locals_, shards, experts, groups, hidden_tile, cols, weight_cuts,
    tok_hbm, mod_hbm, eid_hbm, slot_hbm, emb_hbm, router_hbm, w1_hbm, w2_hbm,
    ret, pick, scale, all_stats,
    tok, mod, eid, slots, emb, router, w1, w2, stage, recv, hid, back, stats, row_stats, row_sum,
    in_sem, w1_sem, w2_sem, go_sem, got_sem, back_sem, ret_sem, stat_send, stat_recv,
):
    devices = nodes * locals_
    half = devices // groups
    width = tok.shape[1]
    count = tok.shape[0]
    chunks = width // cols
    me_n = lax.axis_index("node")
    me_l = lax.axis_index("local")
    me = me_n * locals_ + me_l
    my_pos = (me_n // groups) * locals_ + me_l

    def for_group(group, body):
        def step(i, _):
            peer_n = lax.rem(me_n + (i // locals_) * groups + group, nodes)
            peer_l = lax.rem(me_l + lax.rem(i, locals_), locals_)
            body(peer_n, peer_l)
            return 0

        lax.fori_loop(1 if group == 0 else 0, half, step, 0)

    def all_peers(body):
        for group in range(groups):
            for_group(group, body)

    barrier = pltpu.get_barrier_semaphore()
    all_peers(
        lambda n, l: pl.semaphore_signal(barrier, inc=1, device_id=(n, l), device_id_type=MESH)
    )
    loads = [
        pltpu.make_async_copy(src, dst, in_sem.at[i])
        for i, (src, dst) in enumerate(
            (
                (tok_hbm, tok),
                (mod_hbm, mod),
                (eid_hbm, eid),
                (slot_hbm, slots),
                (emb_hbm, emb),
                (router_hbm, router),
            )
        )
    ]
    for load in loads:
        load.start()
    weight_loads = []
    for hbm, vmem, sem in ((w1_hbm, w1, w1_sem), (w2_hbm, w2, w2_sem)):
        rows = vmem.shape[0] // weight_cuts
        weight_loads.append(
            [
                pltpu.make_async_copy(
                    hbm.at[0, pl.ds(i * rows, rows)], vmem.at[pl.ds(i * rows, rows)], sem.at[i]
                )
                for i in range(weight_cuts)
            ]
        )
    for load in loads:
        load.wait()

    modality = mod[...]
    expert_id = eid[...]
    slot = slots[...]
    is_text = column(modality) == 1
    picked = jnp.where(
        is_text, emb[1:2, :].astype(jnp.float32), emb[0:1, :].astype(jnp.float32)
    )
    mixed = (tok[...].astype(jnp.float32) + picked).astype(jnp.bfloat16)
    place = lax.broadcasted_iota(jnp.int32, (experts * CAP, count), 0)
    select = (place == expert_id * CAP + slot).astype(jnp.bfloat16)
    stage[...] = (
        jnp.dot(select, mixed, preferred_element_type=jnp.float32)
        .reshape(experts, CAP, width)
        .astype(jnp.bfloat16)
    )

    pl.semaphore_wait(barrier, devices - 1)

    for group in range(groups):
        if group == 0:
            pltpu.make_async_copy(
                stage.at[me // shards], recv.at[0, my_pos], got_sem.at[0]
            ).start()

        def dispatch(n, l):
            pltpu.make_async_remote_copy(
                src_ref=stage.at[(n * locals_ + l) // shards],
                dst_ref=recv.at[group, my_pos],
                send_sem=go_sem.at[group],
                recv_sem=got_sem.at[group],
                device_id=(n, l),
                device_id_type=MESH,
            ).start()

        for_group(group, dispatch)

    for weight_load in weight_loads:
        for load in weight_load:
            load.start()

    logits = lax.dot_general(
        mixed, router[...], (((1,), (1,)), ((), ())), preferred_element_type=jnp.float32
    )
    shifted = logits - jnp.max(logits, axis=-1, keepdims=True)
    logp = shifted - jnp.log(jnp.sum(jnp.exp(shifted), axis=-1, keepdims=True))
    probs = jnp.exp(logp)
    entropy = -jnp.sum(probs * logp, axis=-1, keepdims=True)
    expert_col = column(expert_id)
    lane = lax.broadcasted_iota(jnp.int32, (count, experts), 1)
    gate = jnp.sum(jnp.where(lane == expert_col, probs, 0.0), axis=1, keepdims=True)
    stats[...] = jnp.zeros_like(stats)
    for m in range(2):
        member = is_text if m == 1 else jnp.logical_not(is_text)
        stats[m : m + 1, 0:experts] = jnp.sum(
            jnp.where(member, probs, 0.0), axis=0, keepdims=True
        )
        stats[m : m + 1, experts : experts + 1] = jnp.sum(
            jnp.where(member, entropy, 0.0), axis=0, keepdims=True
        )
        stats[m : m + 1, experts + 1 : experts + 2] = jnp.sum(
            jnp.where(member, 1.0, 0.0), axis=0, keepdims=True
        )
    scale[...] = experts * gate
    spot = lax.broadcasted_iota(jnp.int32, (count, devices * CAP), 1)
    first = expert_col * (shards * CAP) + column(slot)
    found = spot == first
    for s in range(1, shards):
        found = jnp.logical_or(found, spot == first + s * CAP)
    pick[...] = found.astype(jnp.bfloat16)

    pltpu.make_async_copy(stats, row_stats.at[me_l], stat_recv.at[0]).start()

    def share_row(i, _):
        pltpu.make_async_remote_copy(
            src_ref=stats,
            dst_ref=row_stats.at[me_l],
            send_sem=stat_send.at[0],
            recv_sem=stat_recv.at[0],
            device_id=(me_n, lax.rem(me_l + i, locals_)),
            device_id_type=MESH,
        ).start()
        return 0

    lax.fori_loop(1, locals_, share_row, 0)

    for group in range(groups):
        pltpu.make_async_copy(recv.at[group], recv.at[group], got_sem.at[group]).wait()
        rows = recv[group].astype(jnp.float32).reshape(half * CAP, width).astype(jnp.bfloat16)
        if group == 0:
            for load in weight_loads[0]:
                load.wait()

        def first_layer(i, _):
            at = pl.ds(pl.multiple_of(i * hidden_tile, hidden_tile), hidden_tile)
            hid[:, at] = gelu(
                jnp.dot(rows, w1[:, at], preferred_element_type=jnp.float32)
            ).astype(jnp.bfloat16)
            return 0

        lax.fori_loop(0, hid.shape[1] // hidden_tile, first_layer, 0)
        if group == 0:
            pltpu.make_async_copy(row_stats, row_stats, stat_recv.at[0]).wait()
            row_sum[...] = jnp.sum(row_stats[...], axis=0)
            for load in weight_loads[1]:
                load.wait()

        def second_layer(c, _):
            at = pl.ds(pl.multiple_of(c * cols, cols), cols)
            back[group, c] = (
                jnp.dot(hid[...], w2[:, at], preferred_element_type=jnp.float32)
                .reshape(half, CAP, cols)
                .astype(jnp.bfloat16)
            )
            if group == 0:
                pltpu.make_async_copy(
                    back.at[0, c, my_pos], ret.at[c, me], ret_sem.at[0, c]
                ).start()

            def give(n, l):
                pltpu.make_async_remote_copy(
                    src_ref=back.at[group, c, (n // groups) * locals_ + l],
                    dst_ref=ret.at[c, me],
                    send_sem=back_sem.at[group, c],
                    recv_sem=ret_sem.at[group, c],
                    device_id=(n, l),
                    device_id_type=MESH,
                ).start()

            for_group(group, give)
            return 0

        lax.fori_loop(0, chunks, second_layer, 0)
        if group == 0:
            pltpu.make_async_copy(row_sum, all_stats.at[me_n], stat_recv.at[1]).start()

            def share_sum(i, _):
                pltpu.make_async_remote_copy(
                    src_ref=row_sum,
                    dst_ref=all_stats.at[me_n],
                    send_sem=stat_send.at[1],
                    recv_sem=stat_recv.at[1],
                    device_id=(lax.rem(me_n + i, nodes), me_l),
                    device_id_type=MESH,
                ).start()
                return 0

            lax.fori_loop(1, nodes, share_sum, 0)

    pltpu.make_async_copy(all_stats, all_stats, stat_recv.at[1]).wait()
    for c in range(chunks):
        for group in range(groups):
            part = ret.at[c, pl.ds(0, half)]
            pltpu.make_async_copy(part, part, ret_sem.at[group, c]).wait()

    for group in range(groups):
        sent = half - 1 if group == 0 else half
        done = recv.at[group, pl.ds(0, sent)]
        pltpu.make_async_copy(done, done, go_sem.at[group]).wait()
        for c in range(chunks):
            done = back.at[group, c, pl.ds(0, sent)]
            pltpu.make_async_copy(done, done, back_sem.at[group, c]).wait()
    for i, done in enumerate(
        (row_stats.at[pl.ds(0, locals_ - 1)], all_stats.at[pl.ds(0, nodes - 1)])
    ):
        pltpu.make_async_copy(done, done, stat_send.at[i]).wait()


def finish(experts, ret, pick, scale, all_stats, out_ref, loss_ref):
    chunks, devices, _, cols = ret.shape
    for c in range(chunks):
        table = (
            ret[c].astype(jnp.float32).reshape(devices * CAP, cols).astype(jnp.bfloat16)
        )
        out_ref[:, c * cols : (c + 1) * cols] = (
            scale[...] * jnp.dot(pick[...], table, preferred_element_type=jnp.float32)
        ).astype(jnp.bfloat16)
    total = jnp.sum(all_stats[...], axis=0)
    tokens_of = total[:, experts + 1 : experts + 2]
    entropy_mean = total[:, experts : experts + 1] / tokens_of
    mean = total[:, 0:experts] / tokens_of
    spread = jnp.sum(mean * jnp.log(mean), axis=1, keepdims=True)
    loss_ref[0] = entropy_mean[0, 0]
    loss_ref[1] = entropy_mean[1, 0]
    loss_ref[2] = spread[0, 0]
    loss_ref[3] = spread[1, 0]


def local(nodes, locals_, tokens, modality, expert_id, slot, type_embed, router, w_in, w_out):
    count, width = tokens.shape
    experts = router.shape[1]
    devices = nodes * locals_
    shards = devices // experts
    hidden = w_in.shape[2]
    groups = GROUPS if nodes % GROUPS == 0 else 1
    half = devices // groups
    cols = width // 2 if width % 256 == 0 else width
    chunks = width // cols
    cuts = 5 if width % 80 == 0 and hidden % 80 == 0 else 1
    bf16 = jnp.bfloat16
    vmem_space = pl.BlockSpec(memory_space=pltpu.VMEM)
    any_space = pl.BlockSpec(memory_space=pl.ANY)
    dma = pltpu.SemaphoreType.DMA
    held = pl.pallas_call(
        functools.partial(
            kernel, nodes, locals_, shards, experts, groups, tile_of(hidden, 512), cols, cuts
        ),
        out_shape=(
            jax.ShapeDtypeStruct((chunks, devices, CAP, cols), bf16),
            jax.ShapeDtypeStruct((count, devices * CAP), bf16),
            jax.ShapeDtypeStruct((count, 1), jnp.float32),
            jax.ShapeDtypeStruct((nodes, 2, LANES), jnp.float32),
        ),
        in_specs=[any_space] * 8,
        out_specs=(vmem_space,) * 4,
        scratch_shapes=[
            pltpu.VMEM((count, width), bf16),
            pltpu.VMEM((1, count), jnp.int32),
            pltpu.VMEM((1, count), jnp.int32),
            pltpu.VMEM((1, count), jnp.int32),
            pltpu.VMEM((2, width), bf16),
            pltpu.VMEM((experts, width), bf16),
            pltpu.VMEM((width, hidden), bf16),
            pltpu.VMEM((hidden, width), bf16),
            pltpu.VMEM((experts, CAP, width), bf16),
            pltpu.VMEM((groups, half, CAP, width), bf16),
            pltpu.VMEM((half * CAP, hidden), bf16),
            pltpu.VMEM((groups, chunks, half, CAP, cols), bf16),
            pltpu.VMEM((2, LANES), jnp.float32),
            pltpu.VMEM((locals_, 2, LANES), jnp.float32),
            pltpu.VMEM((2, LANES), jnp.float32),
            dma((6,)),
            dma((cuts,)),
            dma((cuts,)),
            dma((groups,)),
            dma((groups,)),
            dma((groups, chunks)),
            dma((groups, chunks)),
            dma((2,)),
            dma((2,)),
        ],
        compiler_params=pltpu.CompilerParams(
            collective_id=0, has_side_effects=True, vmem_limit_bytes=62 * 1024 * 1024
        ),
    )(
        tokens,
        modality.reshape(1, count),
        expert_id.reshape(1, count),
        slot.reshape(1, count),
        type_embed,
        router.T,
        w_in,
        w_out,
    )
    return pl.pallas_call(
        functools.partial(finish, experts),
        out_shape=(
            jax.ShapeDtypeStruct((count, width), bf16),
            jax.ShapeDtypeStruct((4,), jnp.float32),
        ),
        in_specs=[vmem_space] * 4,
        out_specs=(vmem_space, pl.BlockSpec(memory_space=pltpu.SMEM)),
    )(*held)


def solution(mesh):
    placed = (
        P(("node", "local"), None),
        P(("node", "local")),
        P(("node", "local")),
        P(("node", "local")),
        P(),
        P(),
        P(("node", "local"), None, None),
        P(("node", "local"), None, None),
    )
    return jax.shard_map(
        functools.partial(local, mesh.shape["node"], mesh.shape["local"]),
        mesh=mesh,
        in_specs=placed,
        out_specs=(P(("node", "local"), None), P()),
        check_vma=False,
    )
```
